256 devices in a mesh: gx: 32 (over x, y, core), gy: 8 (over z).
Axes of the slice: x: 4, y: 4, z: 8, core: 2. Of those that a mesh axis runs over, the one named last changes fastest.
Arguments:
- points: bfloat16 [524288, 64], P(('gx', 'gy')), may hold values from -6 to 6
- order: int32 [256, 2048], P(('gx', 'gy')), may hold values from 0 to 2047, each once within a row
- probes: bfloat16 [524288, 512], P(('gx', 'gy')), may hold values from -6 to 6
- leaf_basis: bfloat16 [524288, 128], P(('gx', 'gy')), may hold values from -0.125 to 0.125
- leaf_transfer: bfloat16 [256, 128, 128], P(('gx', 'gy')), may hold values from -0.4375 to 0.4375
- fine_transfer: bfloat16 [32, 6, 128, 128], P('gx'), may hold values from -0.4375 to 0.4375
- coarse_transfer: bfloat16 [60, 128, 128], replicated, may hold values from -0.4375 to 0.4375
- fine_couple: bfloat16 [32, 7, 2, 128, 128], P('gx'), may hold values from -0.5 to 0.5
- coarse_couple: bfloat16 [31, 2, 128, 128], replicated, may hold values from -0.5 to 0.5
Outputs:
- kernel_product: bfloat16 [524288, 512], P(('gx', 'gy'))
- derivative_product: bfloat16 [524288, 512], P(('gx', 'gy'))
The draws below stay inside these ranges and needn't reach their ends.
Inputs may be any that keep to these rules, and one draw needn't show every extreme that they name: `order`: each row holds every number from 0 to 2047 once.
All inputs are finite; a program needn't handle non-finite values.
Results may differ from the reference program's by a relative error of at most 0.0049.
Values sent between devices are 32-bit elements; how exact they have to be, the bound alone decides.
No kernel may reach another device: no remote copies, remote signals or barrier semaphores. Data moves between devices by JAX's collectives and lax.ppermute only.
A program may use at most 128 MiB of HBM per device.

```python
import jax
import jax.numpy as jnp
from jax import lax

LEAF = 2048
NRHS = 512
FEATURES = 64
RANK = 128
POINTS = 524288
N_GX = 32
N_GY = 8
DEVICES = 256


def block_scale(rng, shape, cuts, low, largest):
    loudness, own = 1.0, jax.random.fold_in(rng, 6)
    for axis_at, parts in cuts:
        draws = jnp.exp(jax.random.uniform(jax.random.fold_in(own, axis_at), (parts,), jnp.float32, low / len(cuts), largest / len(cuts)))
        loudness = loudness * jnp.repeat(draws, shape[axis_at] // parts).reshape([-1 if axis == axis_at else 1 for axis in range(len(shape))])
    return loudness


def normal_values(stream_key, shape, width, most, pieces=(), kind=jnp.bfloat16):
    factor_of = block_scale(stream_key, shape, pieces, -0.22, 0.18) if pieces else 1.0
    values = jax.random.normal(stream_key, shape, jnp.float32) * width * factor_of
    return jnp.minimum(jnp.maximum(values, -most), most).astype(kind)


def setup_inputs(seed: int = 0) -> dict:
    seeds = jax.random.split(jax.random.key(seed), 10)
    return {
        "points": normal_values(seeds[0], (POINTS, FEATURES), 1.0, 6.0, ((0, 256),)),
        "order": jax.vmap(lambda own: jax.random.permutation(own, LEAF))(jax.random.split(seeds[1], DEVICES)).reshape((DEVICES, LEAF)).astype(jnp.int32),
        "probes": normal_values(seeds[2], (POINTS, NRHS), 1.0, 6.0, ((0, 256),)),
        "leaf_basis": normal_values(seeds[3], (POINTS, RANK), LEAF ** -0.5, 0.125, ((0, 256),)),
        "leaf_transfer": normal_values(seeds[4], (DEVICES, RANK, RANK), (1.4142 * RANK) ** -0.5, 0.4375, ((0, 256),)),
        "fine_transfer": normal_values(seeds[5], (N_GX, N_GY - 2, RANK, RANK), (1.4142 * RANK) ** -0.5, 0.4375, ((0, 32),)),
        "coarse_transfer": normal_values(seeds[6], (2 * N_GX - 4, RANK, RANK), (1.4142 * RANK) ** -0.5, 0.4375),
        "fine_couple": normal_values(seeds[7], (N_GX, N_GY - 1, 2, RANK, RANK), RANK ** -0.5, 0.5, ((0, 32),)),
        "coarse_couple": normal_values(seeds[8], (N_GX - 1, 2, RANK, RANK), RANK ** -0.5, 0.5),
    }


length_scale = 3.25

def near_field(cluster_points, cluster_probes):
    leaf_size = cluster_points.shape[0]
    block_rows = min(leaf_size, 512)
    squares = lax.optimization_barrier(jnp.sum(jnp.square(cluster_points.astype(jnp.float32)), axis=1))

    def one_block(offset):
        row_points = lax.dynamic_slice_in_dim(cluster_points, offset, block_rows, 0)
        products = lax.dot_general(row_points, cluster_points, (((1,), (1,)), ((), ())), preferred_element_type=jnp.float32)
        row_squares = lax.dynamic_slice_in_dim(squares, offset, block_rows, 0)
        squared = row_squares[:, None] + squares[None, :] - 2.0 * products
        scaled = jnp.sqrt(3.0 * jnp.maximum(squared, 0.0)) / length_scale
        falloff = jnp.exp(-scaled)
        kernel = ((1.0 + scaled) * falloff).astype(jnp.bfloat16)
        derivative = (scaled * scaled * falloff).astype(jnp.bfloat16)
        stacked = jnp.concatenate([kernel, derivative], axis=0)
        result = jnp.dot(stacked, cluster_probes, preferred_element_type=jnp.float32)
        return result.reshape(2, block_rows, cluster_probes.shape[1])
    offsets = jnp.arange(leaf_size // block_rows, dtype=jnp.int32) * block_rows
    blocks = lax.map(one_block, offsets)
    return jnp.transpose(blocks, (1, 0, 2, 3)).reshape(2, leaf_size, cluster_probes.shape[1])

def log_two(amount):
    return amount.bit_length() - 1

def reference(points, order, probes, leaf_basis, leaf_transfer, fine_transfer, coarse_transfer, fine_couple, coarse_couple):
    exact = lax.Precision.HIGHEST
    leaf_count = order.shape[0]
    leaf_size = order.shape[1]
    rank_size = leaf_basis.shape[1]
    columns = probes.shape[1]
    group_size = N_GY
    group_count = N_GX
    inner_levels = log_two(group_size)
    outer_levels = log_two(group_count)
    levels_all = inner_levels + outer_levels
    cluster_points = jnp.take_along_axis(points.reshape(leaf_count, leaf_size, -1), order[:, :, None], axis=1)
    cluster_probes = jnp.take_along_axis(probes.reshape(leaf_count, leaf_size, -1), order[:, :, None], axis=1)
    basis = leaf_basis.reshape(leaf_count, leaf_size, rank_size)

    def transfer_at(height):
        if height == 0:
            return leaf_transfer.astype(jnp.float32)
        if height < inner_levels:
            offset = group_size - (group_size >> height - 1)
            picked = fine_transfer[:, offset:offset + (group_size >> height)]
            return picked.reshape(-1, rank_size, rank_size).astype(jnp.float32)
        shifted = height - inner_levels
        offset = 2 * group_count - (2 * group_count >> shifted)
        return coarse_transfer[offset:offset + (group_count >> shifted)].astype(jnp.float32)

    def couple_at(height):
        if height < inner_levels:
            offset = group_size - (group_size >> height)
            picked = fine_couple[:, offset:offset + (group_size >> height + 1)]
            return picked.reshape(-1, 2, rank_size, rank_size).astype(jnp.float32)
        shifted = height - inner_levels
        offset = group_count - (group_count >> shifted)
        return coarse_couple[offset:offset + (group_count >> shifted + 1)].astype(jnp.float32)
    coefficient = jnp.einsum('lpr,lpn->lrn', basis.astype(jnp.float32), cluster_probes.astype(jnp.float32), precision=exact)
    upward = [coefficient]
    for height in range(levels_all - 1):
        lifted = jnp.einsum('mrk,mrn->mkn', transfer_at(height), upward[-1], precision=exact)
        upward.append(lifted.reshape(-1, 2, rank_size, columns).sum(axis=1))
    coupled = []
    for height in range(levels_all):
        matrices = couple_at(height)
        values = upward[height]
        left_nodes = values[0::2]
        right_nodes = values[1::2]
        into_left = jnp.einsum('pkrs,psn->pkrn', matrices, right_nodes, precision=exact)
        into_right = jnp.einsum('pksr,psn->pkrn', matrices, left_nodes, precision=exact)
        coupled.append(jnp.stack([into_left, into_right], axis=1).reshape(-1, 2, rank_size, columns))
    descent = coupled[levels_all - 1]
    for height in range(levels_all - 2, -1, -1):
        parent = jnp.repeat(descent, 2, axis=0)
        descent = coupled[height] + jnp.einsum('mrs,mksn->mkrn', transfer_at(height), parent, precision=exact)

    def finish(leaf_items):
        leaf_points, leaf_probes, leaf_base, leaf_coeff = leaf_items
        near_part = near_field(leaf_points, leaf_probes)
        spread = jnp.einsum('pr,krn->kpn', leaf_base.astype(jnp.float32), leaf_coeff, precision=exact)
        return (near_part + spread).astype(jnp.bfloat16)
    combined = lax.map(finish, (cluster_points, cluster_probes, basis, descent))
    return (combined[:, 0].reshape(-1, columns), combined[:, 1].reshape(-1, columns))
```

```python
import functools
import math

import jax
import jax.numpy as jnp
from jax import lax
from jax.experimental import pallas as pl
from jax.experimental.pallas import tpu as pltpu
from jax.sharding import PartitionSpec as P

length_scale = 3.25
bf16 = jnp.bfloat16
f32 = jnp.float32
MIB = 1 << 20


def vmem(count):
    return [pl.BlockSpec(memory_space=pltpu.VMEM)] * count


def held_in_hbm(*arrays):
    return [pltpu.with_memory_space_constraint(array, pltpu.HBM) for array in arrays]


def hbm(count):
    return [pl.BlockSpec(memory_space=pltpu.HBM)] * count


def smem():
    return pl.BlockSpec(memory_space=pltpu.SMEM)


def params(mib):
    return pltpu.CompilerParams(vmem_limit_bytes=mib * MIB)


def cost(flops, moved):
    return pl.CostEstimate(flops=int(flops), bytes_accessed=int(moved), transcendentals=0)


def dot_nn(a, b):
    return lax.dot_general(a, b, (((1,), (0,)), ((), ())), preferred_element_type=f32)


def dot_nt(a, b):
    return lax.dot_general(a, b, (((1,), (1,)), ((), ())), preferred_element_type=f32)


def split(x):
    high = x.astype(bf16)
    low = (x - high.astype(f32)).astype(bf16)
    return jnp.concatenate([high, low], axis=0)


def exact(dot, x, w):
    rows = x.shape[0]
    both = dot(split(x), w)
    return both[:rows] + both[rows:]


def order_columns(order_ref, start, rows):
    pieces = []
    for piece in range(rows // 128):
        line = order_ref[0:1, pl.ds(start + piece * 128, 128)]
        pieces.append(jnp.transpose(jnp.broadcast_to(line, (128, 128))))
    return jnp.concatenate(pieces, axis=0).astype(jnp.int16)


def one_hot(columns, start, width):
    lane = lax.broadcasted_iota(jnp.int32, columns.shape, 1)
    tiles = []
    for tile in range(width // 128):
        lanes = (lane + (start + tile * 128)).astype(jnp.int16)
        tiles.append(jnp.where(columns == lanes, bf16(1.0), bf16(0.0)))
    return jnp.concatenate(tiles, axis=1)


def leaf_up_kernel(
    order_hbm,
    basis_hbm,
    probes_hbm,
    transfer_hbm,
    h_ref,
    lift_ref,
    order_ref,
    basis_ref,
    probes_ref,
    transfer_ref,
    columns_ref,
    hot_ref,
    stored_ref,
    sems,
):
    copies = [
        pltpu.make_async_copy(source, target, sems.at[n])
        for n, (source, target) in enumerate(
            (
                (order_hbm, order_ref),
                (basis_hbm, basis_ref),
                (probes_hbm, probes_ref),
                (transfer_hbm, transfer_ref),
            )
        )
    ]
    for copy in copies:
        copy.start()
    leaf = basis_ref.shape[0]
    step = 512
    copies[0].wait()
    columns_ref[...] = order_columns(order_ref, 0, leaf)
    copies[1].wait()
    basis_t = jnp.transpose(basis_ref[...])
    for start in range(0, leaf, step):
        hot_ref[:, pl.ds(start, step)] = one_hot(columns_ref[...], start, step)
        stored_ref[:, pl.ds(start, step)] = dot_nn(basis_t, hot_ref[:, pl.ds(start, step)]).astype(bf16)
    copies[2].wait()
    h_t = jnp.transpose(dot_nn(stored_ref[...], probes_ref[...]))
    copies[3].wait()
    h_ref[...] = h_t
    lift_ref[...] = exact(dot_nn, h_t, transfer_ref[0])


def leaf_up(order, basis, probes, transfer):
    leaf, rank = basis.shape
    columns = probes.shape[1]
    shape = jax.ShapeDtypeStruct((columns, rank), f32)
    return pl.pallas_call(
        leaf_up_kernel,
        out_shape=(shape, shape),
        in_specs=hbm(4),
        out_specs=tuple(vmem(2)),
        scratch_shapes=[
            pltpu.VMEM(order.shape, order.dtype),
            pltpu.VMEM(basis.shape, bf16),
            pltpu.VMEM(probes.shape, bf16),
            pltpu.VMEM(transfer.shape, bf16),
            pltpu.VMEM((leaf, 128), jnp.int16),
            pltpu.VMEM((leaf, leaf), bf16),
            pltpu.VMEM((rank, leaf), bf16),
            pltpu.SemaphoreType.DMA((4,)),
        ],
        compiler_params=params(24),
        cost_estimate=cost(4e9, 3 * MIB),
        name="leaf_up",
    )(*held_in_hbm(order, basis, probes, transfer))


def near_kernel(order_ref, points_ref, probes_hbm, *refs, first):
    kernel_ref, derivative_ref, right_ref, left_ref, hot_ref, both_ref, probes_ref, sem = refs[-8:]
    features, leaf = points_ref.shape
    rows = kernel_ref.shape[0]
    step = 256
    slope = math.sqrt(3.0) / length_scale
    rate = -slope * math.log2(math.e)
    block = pl.program_id(0)
    copy = pltpu.make_async_copy(probes_hbm, probes_ref, sem)

    @pl.when(block == 0)
    def _():
        copy.start()
        values = points_ref[...].astype(f32)
        norm = jnp.sum(values * values, axis=0, keepdims=True)
        high = norm.astype(bf16).astype(f32)
        rest = norm - high
        middle = rest.astype(bf16).astype(f32)
        low = rest - middle
        line = lax.broadcasted_iota(jnp.int32, (128 - features, leaf), 0)

        def tail(norm_line, ones_line):
            ones = (line >= ones_line) & (line < ones_line + 3)
            out = jnp.where(ones, 1.0, 0.0)
            for offset, piece in enumerate((high, middle, low)):
                out = jnp.where(line == norm_line + offset, piece, out)
            return out

        right_ref[...] = jnp.concatenate([values, tail(0, 3)], axis=0).astype(bf16)
        left_ref[...] = jnp.concatenate([-2.0 * values, tail(3, 0)], axis=0).astype(bf16)
        copy.wait()

    columns = order_columns(order_ref, (first + block) * rows, rows)
    hot_ref[...] = one_hot(columns, 0, leaf)
    rows_left = dot_nt(hot_ref[...], left_ref[...]).astype(bf16)
    for start in range(0, leaf, step):
        squared = dot_nn(rows_left, right_ref[:, pl.ds(start, step)])
        squared = jnp.maximum(squared, 1e-30)
        root = squared * lax.rsqrt(squared)
        falloff = jnp.exp2(root * rate)
        both_ref[0:rows, pl.ds(start, step)] = ((1.0 + root * slope) * falloff).astype(bf16)
        both_ref[rows : 2 * rows, pl.ds(start, step)] = (squared * falloff).astype(bf16)
    sums = dot_nn(both_ref[...], probes_ref[...])
    kernel_ref[...] = sums[:rows].astype(bf16)
    derivative_ref[...] = (sums[rows:] * (slope * slope)).astype(bf16)


def near_part(order, points, probes, held, first, count, rows, name):
    leaf, columns = probes.shape
    shape = pltpu.HBM((leaf, columns), bf16)
    whole = lambda i: (0, 0)
    return pl.pallas_call(
        functools.partial(near_kernel, first=first),
        grid=(count,),
        out_shape=(shape, shape),
        in_specs=[
            pl.BlockSpec(order.shape, whole),
            pl.BlockSpec(points.shape, whole),
            pl.BlockSpec(memory_space=pltpu.HBM),
        ]
        + [pl.BlockSpec(memory_space=pltpu.HBM)] * len(held),
        out_specs=(pl.BlockSpec((rows, columns), lambda i: (first + i, 0)),) * 2,
        scratch_shapes=[
            pltpu.VMEM((128, leaf), bf16),
            pltpu.VMEM((128, leaf), bf16),
            pltpu.VMEM((rows, leaf), bf16),
            pltpu.VMEM((2 * rows, leaf), bf16),
            pltpu.VMEM(probes.shape, bf16),
            pltpu.SemaphoreType.DMA,
        ],
        input_output_aliases={3 + k: k for k in range(len(held))},
        compiler_params=params(36),
        cost_estimate=cost(2.0 * count * rows * leaf * (columns * 2 + 512), 6 * MIB),
        name=name,
    )(order, points, *held_in_hbm(probes, *held))


def fine_up_kernel(lift_ref, transfer_ref, one_ref, two_ref, three_ref):
    twos = []
    for node in range(2):
        total = None
        for child in (2 * node, 2 * node + 1):
            value = lift_ref[2 * child] + lift_ref[2 * child + 1]
            one_ref[child] = value
            moved = exact(dot_nn, value, transfer_ref[0, child])
            total = moved if total is None else total + moved
        two_ref[node] = total
        twos.append(total)
    three_ref[...] = exact(dot_nn, twos[0], transfer_ref[0, 4]) + exact(dot_nn, twos[1], transfer_ref[0, 5])


def fine_up(lifts, transfer):
    columns, rank = lifts.shape[1:]
    return pl.pallas_call(
        fine_up_kernel,
        out_shape=(
            jax.ShapeDtypeStruct((4, columns, rank), f32),
            jax.ShapeDtypeStruct((2, columns, rank), f32),
            jax.ShapeDtypeStruct((columns, rank), f32),
        ),
        in_specs=vmem(2),
        out_specs=tuple(vmem(3)),
        compiler_params=params(8),
        cost_estimate=cost(1e9, MIB),
        name="fine_up",
    )(lifts, transfer)


def pair_up_kernel(place_ref, own_ref, other_ref, transfer_ref, out_ref):
    place = place_ref[0]
    out_ref[...] = exact(dot_nn, own_ref[...], transfer_ref[place]) + exact(
        dot_nn, other_ref[...], transfer_ref[place ^ 1]
    )


def pair_up(place, own, other, transfer):
    return pl.pallas_call(
        pair_up_kernel,
        out_shape=jax.ShapeDtypeStruct(own.shape, f32),
        in_specs=[smem()] + vmem(3),
        out_specs=vmem(1)[0],
        compiler_params=params(8),
        cost_estimate=cost(1e8, MIB // 8),
        name="pair_up",
    )(place, own, other, transfer)


def quad_up_kernel(place_ref, own_ref, x1_ref, x2_ref, x3_ref, transfer_ref, pair_ref, top_ref):
    place = place_ref[0] >> 1
    base = 32
    values = (own_ref, x1_ref, x2_ref, x3_ref)
    moved = [exact(dot_nn, value[...], transfer_ref[base + (place ^ flip)]) for flip, value in enumerate(values)]
    mine = moved[0] + moved[1]
    theirs = moved[2] + moved[3]
    pair_ref[...] = theirs
    place = place >> 1
    base = 48
    top_ref[...] = exact(dot_nn, mine, transfer_ref[base + place]) + exact(
        dot_nn, theirs, transfer_ref[base + (place ^ 1)]
    )


def quad_up(place, own, x1, x2, x3, transfer):
    shape = jax.ShapeDtypeStruct(own.shape, f32)
    return pl.pallas_call(
        quad_up_kernel,
        out_shape=(shape, shape),
        in_specs=[smem()] + vmem(5),
        out_specs=tuple(vmem(2)),
        compiler_params=params(8),
        cost_estimate=cost(1e8, MIB // 8),
        name="quad_up",
    )(place, own, x1, x2, x3, transfer)


def coupled(value, pair_ref, index, side):
    results = []
    for k in range(2):
        matrix = pair_ref[index, k]
        left = exact(dot_nt, value, matrix)
        right = exact(dot_nn, value, matrix)
        results.append(jnp.where(side == 0, left, right))
    return jnp.concatenate(results, axis=0)


def turn_kernel(
    place_ref,
    top_ref,
    x1_ref,
    x2_ref,
    x3_ref,
    five_ref,
    four_ref,
    three_ref,
    two_ref,
    one_ref,
    coarse_ref,
    couple_ref,
    fine_ref,
    fine_couple_ref,
    out_ref,
):
    place = place_ref[0]
    columns = top_ref.shape[0]
    at = place >> 3
    far = exact(dot_nn, x2_ref[...], coarse_ref[56 + (at ^ 2)]) + exact(
        dot_nn, x3_ref[...], coarse_ref[56 + (at ^ 3)]
    )
    z = coupled(far, couple_ref, 30, at >> 1)
    levels = (
        (x1_ref, 28, 56, 3),
        (five_ref, 24, 48, 2),
        (four_ref, 16, 32, 1),
        (three_ref, 0, 0, 0),
    )
    for sibling_ref, couple_base, base, shift in levels:
        at = place >> shift
        g = coupled(sibling_ref[...], couple_ref, couple_base + (at >> 1), at & 1)
        z = g + exact(dot_nt, z, coarse_ref[base + at])
    for node in range(2):
        g = coupled(two_ref[1 - node], fine_couple_ref.at[0], 6, node)
        z_two = g + exact(dot_nt, z, fine_ref[0, 4 + node])
        for child in (2 * node, 2 * node + 1):
            g = coupled(one_ref[child ^ 1], fine_couple_ref.at[0], 4 + node, child & 1)
            z_one = g + exact(dot_nt, z_two, fine_ref[0, child])
            out_ref[2 * child] = z_one
            out_ref[2 * child + 1] = z_one


def turn(place, *operands):
    columns, rank = operands[0].shape
    return pl.pallas_call(
        turn_kernel,
        out_shape=jax.ShapeDtypeStruct((8, 2 * columns, rank), f32),
        in_specs=[smem()] + vmem(len(operands)),
        out_specs=vmem(1)[0],
        compiler_params=params(16),
        cost_estimate=cost(1e9, MIB),
        name="turn",
    )(place, *operands)


def leaf_couple_kernel(place_ref, sibling_ref, couple_ref, out_ref):
    place = place_ref[1]
    columns = sibling_ref.shape[0]
    g = coupled(sibling_ref[...], couple_ref.at[0], place >> 1, place & 1)
    out_ref[0] = g[:columns]
    out_ref[1] = g[columns:]


def leaf_couple(place, sibling, couple):
    columns, rank = sibling.shape
    return pl.pallas_call(
        leaf_couple_kernel,
        out_shape=jax.ShapeDtypeStruct((2, columns, rank), f32),
        in_specs=[smem()] + vmem(2),
        out_specs=vmem(1)[0],
        compiler_params=params(16),
        cost_estimate=cost(1e9, MIB),
        name="leaf_couple",
    )(place, sibling, couple)


def finish_kernel(down_ref, couple_ref, transfer_ref, basis_ref, near_k_ref, near_d_ref, out_k_ref, out_d_ref, z_ref):
    columns = couple_ref.shape[1]
    part = down_ref.shape[1] // 2

    @pl.when(pl.program_id(0) == 0)
    def _():
        for k in range(2):
            parent = jnp.concatenate([down_ref[s, k * part : (k + 1) * part] for s in range(down_ref.shape[0])], axis=0)
            z = couple_ref[k] + exact(dot_nt, parent, transfer_ref[0])
            z_ref[k] = z.astype(bf16)

    basis = basis_ref[...]
    out_k_ref[...] = (near_k_ref[...].astype(f32) + dot_nt(basis, z_ref[0])).astype(bf16)
    out_d_ref[...] = (near_d_ref[...].astype(f32) + dot_nt(basis, z_ref[1])).astype(bf16)


def finish(down, couple, transfer, basis, near_k, near_d, rows):
    leaf, columns = near_k.shape
    rank = basis.shape[1]
    shape = jax.ShapeDtypeStruct((leaf, columns), bf16)
    tile = pl.BlockSpec((rows, columns), lambda i: (i, 0))
    return pl.pallas_call(
        finish_kernel,
        grid=(leaf // rows,),
        out_shape=(shape, shape),
        in_specs=[
            pl.BlockSpec(down.shape, lambda i: (0, 0, 0)),
            pl.BlockSpec(couple.shape, lambda i: (0, 0, 0)),
            pl.BlockSpec(transfer.shape, lambda i: (0, 0, 0)),
            pl.BlockSpec((rows, rank), lambda i: (i, 0)),
            tile,
            tile,
        ],
        out_specs=(tile, tile),
        scratch_shapes=[pltpu.VMEM((2, columns, rank), bf16)],
        compiler_params=params(24),
        cost_estimate=cost(1e9, 10 * MIB),
        name="finish",
    )(down, couple, transfer, *held_in_hbm(basis, near_k, near_d))


def swap(x, axis, mask):
    return lax.ppermute(x, axis, [(i, i ^ mask) for i in range(lax.axis_size(axis))])


def per_device(
    points, order, probes, leaf_basis, leaf_transfer, fine_transfer, coarse_transfer, fine_couple, coarse_couple
):
    group = lax.axis_size("gy")
    place = jnp.stack([lax.axis_index("gx"), lax.axis_index("gy")]).astype(jnp.int32)
    points_t = jnp.transpose(points)
    h_t, lift_t = leaf_up(order, leaf_basis, probes, leaf_transfer)
    columns, rank = h_t.shape
    order_a, lift_t = lax.optimization_barrier((order, lift_t))
    lifts = lax.all_to_all(lift_t.reshape(group, columns // group, rank), "gy", 0, 0)
    near_a = near_part(order_a, points_t, probes, (), 0, 2, 512, "near_a")
    near_a, lifts = lax.optimization_barrier((near_a, lifts))
    one, two, three = fine_up(lifts, fine_transfer)
    leaf_sibling = swap(h_t, "gy", 1)
    three_sibling = swap(three, "gx", 1)
    four = pair_up(place, three, three_sibling, coarse_transfer)
    y1, y2, y3 = [swap(four, "gx", mask << 1) for mask in (1, 2, 3)]
    five_sibling, six = quad_up(place, four, y1, y2, y3, coarse_transfer)
    x1, x2, x3 = [swap(six, "gx", mask << 3) for mask in (1, 2, 3)]
    sent = turn(
        place,
        six,
        x1,
        x2,
        x3,
        five_sibling,
        y1,
        three_sibling,
        two,
        one,
        coarse_transfer,
        coarse_couple,
        fine_transfer,
        fine_couple,
    )
    order_b, sent = lax.optimization_barrier((order, sent))
    down = lax.all_to_all(sent, "gy", 0, 0)
    near = near_part(order_b, points_t, probes, near_a, 2, 2, 512, "near_b")
    leaf_g = leaf_couple(place, leaf_sibling, fine_couple)
    return finish(down, leaf_g, leaf_transfer, leaf_basis, near[0], near[1], 256)


def solution(mesh):
    placed = (
        P(("gx", "gy"), None),
        P(("gx", "gy"), None),
        P(("gx", "gy"), None),
        P(("gx", "gy"), None),
        P(("gx", "gy"), None, None),
        P("gx", None, None, None),
        P(),
        P("gx", None, None, None, None),
        P(),
    )
    return jax.shard_map(
        per_device,
        mesh=mesh,
        in_specs=placed,
        out_specs=(P(("gx", "gy"), None), P(("gx", "gy"), None)),
        check_vma=False,
    )
```

```python
import functools
import math

import jax
import jax.numpy as jnp
from jax import lax
from jax.experimental import pallas as pl
from jax.experimental.pallas import tpu as pltpu
from jax.sharding import PartitionSpec as P


length_scale = 3.25
bf16 = jnp.bfloat16
f32 = jnp.float32
MIB = 1 << 20


def vmem(count):
    return [pl.BlockSpec(memory_space=pltpu.VMEM)] * count


def held_in_hbm(*arrays):
    return [pltpu.with_memory_space_constraint(array, pltpu.HBM) for array in arrays]


def hbm(count):
    return [pl.BlockSpec(memory_space=pltpu.HBM)] * count


def smem():
    return pl.BlockSpec(memory_space=pltpu.SMEM)


def params(mib):
    return pltpu.CompilerParams(vmem_limit_bytes=mib * MIB)


def cost(flops, moved):
    return pl.CostEstimate(flops=int(flops), bytes_accessed=int(moved), transcendentals=0)


def dot_nn(a, b):
    return lax.dot_general(a, b, (((1,), (0,)), ((), ())), preferred_element_type=f32)


def dot_nt(a, b):
    return lax.dot_general(a, b, (((1,), (1,)), ((), ())), preferred_element_type=f32)


def split(x):
    high = x.astype(bf16)
    low = (x - high.astype(f32)).astype(bf16)
    return jnp.concatenate([high, low], axis=0)


def exact(dot, x, w):
    rows = x.shape[0]
    both = dot(split(x), w)
    return both[:rows] + both[rows:]


def order_columns(order_ref, start, rows):
    pieces = []
    for piece in range(rows // 128):
        line = order_ref[0:1, pl.ds(start + piece * 128, 128)]
        pieces.append(jnp.transpose(jnp.broadcast_to(line, (128, 128))))
    return jnp.concatenate(pieces, axis=0).astype(jnp.int16)


def one_hot(columns, start, width):
    lane = lax.broadcasted_iota(jnp.int32, columns.shape, 1)
    tiles = []
    for tile in range(width // 128):
        lanes = (lane + (start + tile * 128)).astype(jnp.int16)
        tiles.append(jnp.where(columns == lanes, bf16(1.0), bf16(0.0)))
    return jnp.concatenate(tiles, axis=1)


def leaf_up_kernel(
    order_hbm,
    basis_hbm,
    probes_hbm,
    transfer_hbm,
    h_ref,
    lift_ref,
    order_ref,
    basis_ref,
    probes_ref,
    transfer_ref,
    columns_ref,
    hot_ref,
    stored_ref,
    sems,
):
    copies = [
        pltpu.make_async_copy(source, target, sems.at[n])
        for n, (source, target) in enumerate(
            (
                (order_hbm, order_ref),
                (basis_hbm, basis_ref),
                (probes_hbm, probes_ref),
                (transfer_hbm, transfer_ref),
            )
        )
    ]
    for copy in copies:
        copy.start()
    leaf = basis_ref.shape[0]
    step = 512
    copies[0].wait()
    columns_ref[...] = order_columns(order_ref, 0, leaf)
    copies[1].wait()
    basis_t = jnp.transpose(basis_ref[...])
    for start in range(0, leaf, step):
        hot_ref[:, pl.ds(start, step)] = one_hot(columns_ref[...], start, step)
        stored_ref[:, pl.ds(start, step)] = dot_nn(basis_t, hot_ref[:, pl.ds(start, step)]).astype(bf16)
    copies[2].wait()
    h_t = jnp.transpose(dot_nn(stored_ref[...], probes_ref[...]))
    copies[3].wait()
    h_ref[...] = h_t
    lift_ref[...] = exact(dot_nn, h_t, transfer_ref[0])


def leaf_up(order, basis, probes, transfer):
    leaf, rank = basis.shape
    columns = probes.shape[1]
    shape = jax.ShapeDtypeStruct((columns, rank), f32)
    return pl.pallas_call(
        leaf_up_kernel,
        out_shape=(shape, shape),
        in_specs=hbm(4),
        out_specs=tuple(vmem(2)),
        scratch_shapes=[
            pltpu.VMEM(order.shape, order.dtype),
            pltpu.VMEM(basis.shape, bf16),
            pltpu.VMEM(probes.shape, bf16),
            pltpu.VMEM(transfer.shape, bf16),
            pltpu.VMEM((leaf, 128), jnp.int16),
            pltpu.VMEM((leaf, leaf), bf16),
            pltpu.VMEM((rank, leaf), bf16),
            pltpu.SemaphoreType.DMA((4,)),
        ],
        compiler_params=params(24),
        cost_estimate=cost(4e9, 3 * MIB),
        name="leaf_up",
    )(*held_in_hbm(order, basis, probes, transfer))


def near_kernel(order_ref, points_ref, transfer_ref, basis_ref, probes_hbm, *refs, first):
    extra = refs[:3] if len(refs) > 10 else None
    outs, (right_ref, left_ref, hot_ref, both_ref, probes_ref, sem) = refs[:-6], refs[-6:]
    kernel_ref, derivative_ref, wide_ref = outs[len(outs) - 3 :] if extra is None else outs[3:6]
    features, leaf = points_ref.shape
    rows = kernel_ref.shape[0]
    step = 256
    slope = math.sqrt(3.0) / length_scale
    rate = -slope * math.log2(math.e)
    block = pl.program_id(0)
    copy = pltpu.make_async_copy(probes_hbm, probes_ref, sem)

    @pl.when(block == 0)
    def _():
        copy.start()
        values = points_ref[...].astype(f32)
        norm = jnp.sum(values * values, axis=0, keepdims=True)
        high = norm.astype(bf16).astype(f32)
        rest = norm - high
        middle = rest.astype(bf16).astype(f32)
        low = rest - middle
        line = lax.broadcasted_iota(jnp.int32, (128 - features, leaf), 0)

        def tail(norm_line, ones_line):
            ones = (line >= ones_line) & (line < ones_line + 3)
            out = jnp.where(ones, 1.0, 0.0)
            for offset, piece in enumerate((high, middle, low)):
                out = jnp.where(line == norm_line + offset, piece, out)
            return out

        right_ref[...] = jnp.concatenate([values, tail(0, 3)], axis=0).astype(bf16)
        left_ref[...] = jnp.concatenate([-2.0 * values, tail(3, 0)], axis=0).astype(bf16)
        if extra is not None:
            place_ref, sibling_ref, couple_ref = extra
            place = place_ref[1]
            size = sibling_ref.shape[0]
            g = coupled(sibling_ref[...], couple_ref.at[0], place >> 1, place & 1).astype(bf16)
            outs[6][0] = g[:size]
            outs[6][1] = g[size:]

    columns = order_columns(order_ref, first + block * rows, rows)
    hot_ref[...] = one_hot(columns, 0, leaf)
    rows_left = dot_nt(hot_ref[...], left_ref[...]).astype(bf16)
    basis = basis_ref[...]
    rank = basis.shape[1]
    wide_ref[:, :rank] = dot_nn(basis, transfer_ref[0]).astype(bf16)
    wide_ref[:, rank:] = basis
    for start in range(0, leaf, step):
        squared = dot_nn(rows_left, right_ref[:, pl.ds(start, step)])
        squared = jnp.maximum(squared, 1e-30)
        root = squared * lax.rsqrt(squared)
        falloff = jnp.exp2(root * rate)
        both_ref[0:rows, pl.ds(start, step)] = ((1.0 + root * slope) * falloff).astype(bf16)
        both_ref[rows : 2 * rows, pl.ds(start, step)] = (squared * falloff).astype(bf16)

    @pl.when(block == 0)
    def _():
        copy.wait()

    sums = dot_nn(both_ref[...], probes_ref[...])
    kernel_ref[...] = sums[:rows].astype(bf16)
    derivative_ref[...] = (sums[rows:] * (slope * slope)).astype(bf16)


def near_part(order, points, transfer, basis, probes, extra, first, count, rows):
    leaf, columns = probes.shape
    rank = basis.shape[1]
    held = first // rows
    out_shape = [pltpu.HBM((count * rows, width), bf16) for width in (columns, columns, 2 * rank)]
    out_specs = [pl.BlockSpec((rows, width), lambda i: (i, 0)) for width in (columns, columns, 2 * rank)]
    extra_specs = []
    if extra:
        out_shape.append(pltpu.HBM((2, columns, rank), bf16))
        out_specs.append(pl.BlockSpec((2, columns, rank), lambda i: (0, 0, 0)))
        extra_specs = [smem()] + [
            pl.BlockSpec(array.shape, functools.partial(lambda n, i: (0,) * n, array.ndim)) for array in extra[1:]
        ]
    whole = lambda i: (0, 0)
    return pl.pallas_call(
        functools.partial(near_kernel, first=first),
        grid=(count,),
        out_shape=tuple(out_shape),
        in_specs=[
            pl.BlockSpec(order.shape, whole),
            pl.BlockSpec(points.shape, whole),
            pl.BlockSpec(transfer.shape, lambda i: (0, 0, 0)),
            pl.BlockSpec((rows, rank), lambda i: (held + i, 0)),
            pl.BlockSpec(memory_space=pltpu.HBM),
        ]
        + extra_specs,
        out_specs=tuple(out_specs),
        scratch_shapes=[
            pltpu.VMEM((128, leaf), bf16),
            pltpu.VMEM((128, leaf), bf16),
            pltpu.VMEM((rows, leaf), bf16),
            pltpu.VMEM((2 * rows, leaf), bf16),
            pltpu.VMEM(probes.shape, bf16),
            pltpu.SemaphoreType.DMA,
        ],
        compiler_params=params(32),
        cost_estimate=cost(2.0 * count * rows * leaf * (columns * 2 + 512), 6 * MIB),
    )(order, points, transfer, *held_in_hbm(basis, probes), *extra)


def fine_up_kernel(lift_ref, transfer_ref, one_ref, two_ref, three_ref):
    twos = []
    for node in range(2):
        total = None
        for child in (2 * node, 2 * node + 1):
            value = lift_ref[2 * child] + lift_ref[2 * child + 1]
            one_ref[child] = value
            moved = exact(dot_nn, value, transfer_ref[0, child])
            total = moved if total is None else total + moved
        two_ref[node] = total
        twos.append(total)
    three_ref[...] = exact(dot_nn, twos[0], transfer_ref[0, 4]) + exact(dot_nn, twos[1], transfer_ref[0, 5])


def fine_up(lifts, transfer):
    columns, rank = lifts.shape[1:]
    return pl.pallas_call(
        fine_up_kernel,
        out_shape=(
            jax.ShapeDtypeStruct((4, columns, rank), f32),
            jax.ShapeDtypeStruct((2, columns, rank), f32),
            jax.ShapeDtypeStruct((columns, rank), f32),
        ),
        in_specs=vmem(2),
        out_specs=tuple(vmem(3)),
        compiler_params=params(8),
        cost_estimate=cost(1e9, MIB),
        name="fine_up",
    )(lifts, transfer)


def pair_up_kernel(place_ref, own_ref, other_ref, transfer_ref, out_ref):
    place = place_ref[0]
    out_ref[...] = exact(dot_nn, own_ref[...], transfer_ref[place]) + exact(
        dot_nn, other_ref[...], transfer_ref[place ^ 1]
    )


def pair_up(place, own, other, transfer):
    return pl.pallas_call(
        pair_up_kernel,
        out_shape=jax.ShapeDtypeStruct(own.shape, f32),
        in_specs=[smem()] + vmem(3),
        out_specs=vmem(1)[0],
        compiler_params=params(8),
        cost_estimate=cost(1e8, MIB // 8),
        name="pair_up",
    )(place, own, other, transfer)


def quad_up_kernel(place_ref, own_ref, x1_ref, x2_ref, x3_ref, transfer_ref, pair_ref, top_ref):
    place = place_ref[0] >> 1
    base = 32
    values = (own_ref, x1_ref, x2_ref, x3_ref)
    moved = [exact(dot_nn, value[...], transfer_ref[base + (place ^ flip)]) for flip, value in enumerate(values)]
    mine = moved[0] + moved[1]
    theirs = moved[2] + moved[3]
    pair_ref[...] = theirs
    place = place >> 1
    base = 48
    top_ref[...] = exact(dot_nn, mine, transfer_ref[base + place]) + exact(
        dot_nn, theirs, transfer_ref[base + (place ^ 1)]
    )


def quad_up(place, own, x1, x2, x3, transfer):
    shape = jax.ShapeDtypeStruct(own.shape, f32)
    return pl.pallas_call(
        quad_up_kernel,
        out_shape=(shape, shape),
        in_specs=[smem()] + vmem(5),
        out_specs=tuple(vmem(2)),
        compiler_params=params(8),
        cost_estimate=cost(1e8, MIB // 8),
        name="quad_up",
    )(place, own, x1, x2, x3, transfer)


def coupled(value, pair_ref, index, side):
    rank = value.shape[1]
    sides = []
    for k in range(2):
        matrix = pair_ref[index, k].astype(f32)
        sides.append(jnp.where(side == 0, jnp.transpose(matrix), matrix).astype(bf16))
    both = exact(dot_nn, value, jnp.concatenate(sides, axis=1))
    return jnp.concatenate([both[:, :rank], both[:, rank:]], axis=0)


def turn_kernel(
    place_ref,
    top_ref,
    x1_ref,
    x2_ref,
    x3_ref,
    five_ref,
    four_ref,
    three_ref,
    two_ref,
    one_ref,
    coarse_ref,
    couple_ref,
    fine_ref,
    fine_couple_ref,
    out_ref,
):
    place = place_ref[0]
    at = place >> 3
    far = exact(dot_nn, x2_ref[...], coarse_ref[56 + (at ^ 2)]) + exact(
        dot_nn, x3_ref[...], coarse_ref[56 + (at ^ 3)]
    )
    z = coupled(far, couple_ref, 30, at >> 1)
    levels = (
        (x1_ref, 28, 56, 3),
        (five_ref, 24, 48, 2),
        (four_ref, 16, 32, 1),
        (three_ref, 0, 0, 0),
    )
    for sibling_ref, couple_base, base, shift in levels:
        at = place >> shift
        g = coupled(sibling_ref[...], couple_ref, couple_base + (at >> 1), at & 1)
        z = g + exact(dot_nt, z, coarse_ref[base + at])
    for node in range(2):
        g = coupled(two_ref[1 - node], fine_couple_ref.at[0], 6, node)
        z_two = g + exact(dot_nt, z, fine_ref[0, 4 + node])
        for child in (2 * node, 2 * node + 1):
            g = coupled(one_ref[child ^ 1], fine_couple_ref.at[0], 4 + node, child & 1)
            z_one = g + exact(dot_nt, z_two, fine_ref[0, child])
            out_ref[2 * child] = z_one
            out_ref[2 * child + 1] = z_one


def turn(place, *operands):
    columns, rank = operands[0].shape
    return pl.pallas_call(
        turn_kernel,
        out_shape=jax.ShapeDtypeStruct((8, 2 * columns, rank), f32),
        in_specs=[smem()] + vmem(len(operands)),
        out_specs=vmem(1)[0],
        compiler_params=params(16),
        cost_estimate=cost(1e9, MIB),
        name="turn",
    )(place, *operands)


def finish_kernel(down_ref, couple_hbm, *refs):
    parts_hbm = refs[:6]
    out_k_hbm, out_d_hbm, couple_ref, wide_ref, near_ref, held_ref, in_sems, out_sems = refs[6:]
    part = down_ref.shape[1] // 2
    arrivals = [pltpu.make_async_copy(couple_hbm, couple_ref, in_sems.at[0])]
    spans = []
    start = 0
    for half in range(2):
        near_k, near_d, wide = parts_hbm[3 * half : 3 * half + 3]
        span = pl.ds(start, near_k.shape[0])
        spans.append(span)
        start += near_k.shape[0]
        for source, target in (
            (wide, wide_ref.at[span, :]),
            (near_k, near_ref.at[0, span, :]),
            (near_d, near_ref.at[1, span, :]),
        ):
            arrivals.append(pltpu.make_async_copy(source, target, in_sems.at[len(arrivals)]))
    for copy in arrivals:
        copy.start()
    parents = [
        jnp.concatenate([down_ref[s, k * part : (k + 1) * part].astype(bf16) for s in range(down_ref.shape[0])], axis=0)
        for k in range(2)
    ]
    arrivals[0].wait()
    both = [jnp.concatenate([parents[k], couple_ref[k]], axis=1) for k in range(2)]
    departures = []
    for half, span in enumerate(spans):
        arrivals[1 + 3 * half].wait()
        for k, out_hbm in enumerate((out_k_hbm, out_d_hbm)):
            arrivals[2 + 3 * half + k].wait()
            far = dot_nt(wide_ref[span, :], both[k])
            held_ref[k, span, :] = (near_ref[k, span, :].astype(f32) + far).astype(bf16)
            departures.append(
                pltpu.make_async_copy(held_ref.at[k, span, :], out_hbm.at[span, :], out_sems.at[len(departures)])
            )
            departures[-1].start()
    for copy in departures:
        copy.wait()


def finish(down, couple, *parts):
    leaf = parts[0].shape[0] + parts[3].shape[0]
    columns = parts[0].shape[1]
    wide = parts[2].shape[1]
    shape = jax.ShapeDtypeStruct((leaf, columns), bf16)
    return pl.pallas_call(
        finish_kernel,
        out_shape=(shape, shape),
        in_specs=vmem(1) + hbm(1 + len(parts)),
        out_specs=tuple(hbm(2)),
        scratch_shapes=[
            pltpu.VMEM(couple.shape, bf16),
            pltpu.VMEM((leaf, wide), bf16),
            pltpu.VMEM((2, leaf, columns), bf16),
            pltpu.VMEM((2, leaf, columns), bf16),
            pltpu.SemaphoreType.DMA((7,)),
            pltpu.SemaphoreType.DMA((4,)),
        ],
        compiler_params=params(24),
        cost_estimate=cost(1e9, 10 * MIB),
        name="finish",
    )(down, *held_in_hbm(couple, *parts))


def swap(x, axis, mask):
    return lax.ppermute(x, axis, [(i, i ^ mask) for i in range(lax.axis_size(axis))])


def per_device(
    points, order, probes, leaf_basis, leaf_transfer, fine_transfer, coarse_transfer, fine_couple, coarse_couple
):
    group = lax.axis_size("gy")
    place = jnp.stack([lax.axis_index("gx"), lax.axis_index("gy")]).astype(jnp.int32)
    points_t = jnp.transpose(points)
    h_t, lift_t = leaf_up(order, leaf_basis, probes, leaf_transfer)
    columns, rank = h_t.shape
    leaf = probes.shape[0]
    order_a, lift_t = lax.optimization_barrier((order, lift_t))
    lifts = lax.all_to_all(lift_t.reshape(group, columns // group, rank), "gy", 0, 0)
    rows = leaf // 4
    near_a = near_part(order_a, points_t, leaf_transfer, leaf_basis, probes, (), 0, 2, rows)
    near_a, lifts = lax.optimization_barrier((near_a, lifts))
    one, two, three = fine_up(lifts, fine_transfer)
    three_sibling = swap(three, "gx", 1)
    four = pair_up(place, three, three_sibling, coarse_transfer)
    four, h_t = lax.optimization_barrier((four, h_t))
    y1, y2, y3 = [swap(four, "gx", mask << 1) for mask in (1, 2, 3)]
    leaf_sibling = swap(h_t, "gy", 1)
    five_sibling, six = quad_up(place, four, y1, y2, y3, coarse_transfer)
    x1, x2, x3 = [swap(six, "gx", mask << 3) for mask in (1, 2, 3)]
    sent = turn(
        place,
        six,
        x1,
        x2,
        x3,
        five_sibling,
        y1,
        three_sibling,
        two,
        one,
        coarse_transfer,
        coarse_couple,
        fine_transfer,
        fine_couple,
    )
    order_b, leaf_sibling, sent = lax.optimization_barrier((order, leaf_sibling, sent))
    down = lax.all_to_all(sent, "gy", 0, 0)
    extra = (place, leaf_sibling, fine_couple)
    near_b = near_part(order_b, points_t, leaf_transfer, leaf_basis, probes, extra, 2 * rows, 2, rows)
    return finish(down, near_b[3], *near_a, *near_b[:3])


def solution(mesh):
    placed = (
        P(("gx", "gy"), None),
        P(("gx", "gy"), None),
        P(("gx", "gy"), None),
        P(("gx", "gy"), None),
        P(("gx", "gy"), None, None),
        P("gx", None, None, None),
        P(),
        P("gx", None, None, None, None),
        P(),
    )
    return jax.shard_map(
        per_device,
        mesh=mesh,
        in_specs=placed,
        out_specs=(P(("gx", "gy"), None), P(("gx", "gy"), None)),
        check_vma=False,
    )
```

```python
import functools
import math

import jax
import jax.numpy as jnp
from jax import lax
from jax.experimental import pallas as pl
from jax.experimental.pallas import tpu as pltpu
from jax.sharding import PartitionSpec as P


length_scale = 3.25
bf16 = jnp.bfloat16
f32 = jnp.float32
MIB = 1 << 20


def vmem(count):
    return [pl.BlockSpec(memory_space=pltpu.VMEM)] * count


def held_in_hbm(*arrays):
    return [pltpu.with_memory_space_constraint(array, pltpu.HBM) for array in arrays]


def hbm(count):
    return [pl.BlockSpec(memory_space=pltpu.HBM)] * count


def smem():
    return pl.BlockSpec(memory_space=pltpu.SMEM)


def params(mib):
    return pltpu.CompilerParams(vmem_limit_bytes=mib * MIB)


def cost(flops, moved):
    return pl.CostEstimate(flops=int(flops), bytes_accessed=int(moved), transcendentals=0)


def dot_nn(a, b):
    return lax.dot_general(a, b, (((1,), (0,)), ((), ())), preferred_element_type=f32)


def dot_nt(a, b):
    return lax.dot_general(a, b, (((1,), (1,)), ((), ())), preferred_element_type=f32)


def split(x):
    high = x.astype(bf16)
    low = (x - high.astype(f32)).astype(bf16)
    return jnp.concatenate([high, low], axis=0)


def exact(dot, x, w):
    rows = x.shape[0]
    both = dot(split(x), w)
    return both[:rows] + both[rows:]


def order_columns(order_ref, start, rows):
    pieces = []
    for piece in range(rows // 128):
        line = order_ref[0:1, pl.ds(start + piece * 128, 128)]
        pieces.append(jnp.transpose(jnp.broadcast_to(line, (128, 128))))
    return jnp.concatenate(pieces, axis=0).astype(jnp.int16)


def one_hot(columns, start, width):
    lane = lax.broadcasted_iota(jnp.int32, columns.shape, 1)
    tiles = []
    for tile in range(width // 128):
        lanes = (lane + (start + tile * 128)).astype(jnp.int16)
        tiles.append(jnp.where(columns == lanes, bf16(1.0), bf16(0.0)))
    return jnp.concatenate(tiles, axis=1)


def leaf_up_kernel(
    order_hbm,
    basis_hbm,
    probes_hbm,
    transfer_hbm,
    h_ref,
    lift_ref,
    order_ref,
    basis_ref,
    probes_ref,
    transfer_ref,
    columns_ref,
    hot_ref,
    stored_ref,
    sems,
):
    copies = [
        pltpu.make_async_copy(source, target, sems.at[n])
        for n, (source, target) in enumerate(
            (
                (order_hbm, order_ref),
                (basis_hbm, basis_ref),
                (probes_hbm, probes_ref),
                (transfer_hbm, transfer_ref),
            )
        )
    ]
    for copy in copies:
        copy.start()
    leaf = basis_ref.shape[0]
    step = 512
    copies[0].wait()
    columns_ref[...] = order_columns(order_ref, 0, leaf)
    copies[1].wait()
    basis_t = jnp.transpose(basis_ref[...])
    for start in range(0, leaf, step):
        hot_ref[:, pl.ds(start, step)] = one_hot(columns_ref[...], start, step)
        stored_ref[:, pl.ds(start, step)] = dot_nn(basis_t, hot_ref[:, pl.ds(start, step)]).astype(bf16)
    copies[2].wait()
    h_t = jnp.transpose(dot_nn(stored_ref[...], probes_ref[...]))
    copies[3].wait()
    h_ref[...] = h_t
    half = h_t.shape[0] // 2
    for part in (0, half):
        lift_ref[part : part + half, :] = exact(dot_nn, h_t[part : part + half], transfer_ref[0])


def leaf_up(order, basis, probes, transfer):
    leaf, rank = basis.shape
    columns = probes.shape[1]
    shape = jax.ShapeDtypeStruct((columns, rank), f32)
    return pl.pallas_call(
        leaf_up_kernel,
        out_shape=(shape, shape),
        in_specs=hbm(4),
        out_specs=tuple(vmem(2)),
        scratch_shapes=[
            pltpu.VMEM(order.shape, order.dtype),
            pltpu.VMEM(basis.shape, bf16),
            pltpu.VMEM(probes.shape, bf16),
            pltpu.VMEM(transfer.shape, bf16),
            pltpu.VMEM((leaf, 128), jnp.int16),
            pltpu.VMEM((leaf, leaf), bf16),
            pltpu.VMEM((rank, leaf), bf16),
            pltpu.SemaphoreType.DMA((4,)),
        ],
        compiler_params=params(24),
        cost_estimate=cost(4e9, 3 * MIB),
        name="leaf_up",
    )(*held_in_hbm(order, basis, probes, transfer))


def near_kernel(order_ref, points_ref, transfer_ref, basis_ref, probes_hbm, *refs, first):
    extra = refs[:3] if len(refs) > 10 else None
    outs, (right_ref, left_ref, hot_ref, both_ref, probes_ref, sem) = refs[:-6], refs[-6:]
    kernel_ref, derivative_ref, wide_ref = outs[len(outs) - 3 :] if extra is None else outs[3:6]
    features, leaf = points_ref.shape
    rows = kernel_ref.shape[0]
    step = 256
    slope = math.sqrt(3.0) / length_scale
    rate = -slope * math.log2(math.e)
    block = pl.program_id(0)
    copy = pltpu.make_async_copy(probes_hbm, probes_ref, sem)

    @pl.when(block == 0)
    def _():
        copy.start()
        values = points_ref[...].astype(f32)
        norm = jnp.sum(values * values, axis=0, keepdims=True)
        high = norm.astype(bf16).astype(f32)
        rest = norm - high
        middle = rest.astype(bf16).astype(f32)
        low = rest - middle
        line = lax.broadcasted_iota(jnp.int32, (128 - features, leaf), 0)

        def tail(norm_line, ones_line):
            ones = (line >= ones_line) & (line < ones_line + 3)
            out = jnp.where(ones, 1.0, 0.0)
            for offset, piece in enumerate((high, middle, low)):
                out = jnp.where(line == norm_line + offset, piece, out)
            return out

        right_ref[...] = jnp.concatenate([values, tail(0, 3)], axis=0).astype(bf16)
        left_ref[...] = jnp.concatenate([-2.0 * values, tail(3, 0)], axis=0).astype(bf16)
        if extra is not None:
            place_ref, sibling_ref, couple_ref = extra
            place = place_ref[1]
            size = sibling_ref.shape[0]
            g = coupled(sibling_ref[...], couple_ref.at[0], place >> 1, place & 1).astype(bf16)
            outs[6][0] = g[:size]
            outs[6][1] = g[size:]

    columns = order_columns(order_ref, first + block * rows, rows)
    hot_ref[...] = one_hot(columns, 0, leaf)
    half = rows // 2
    rows_left = jnp.concatenate(
        [dot_nt(hot_ref[part : part + half, :], left_ref[...]) for part in (0, half)], axis=0
    ).astype(bf16)

    @pl.when(block == 0)
    def _():
        copy.wait()

    basis = basis_ref[pl.ds(pl.multiple_of(first + block * rows, 128), rows), :]
    rank = basis.shape[1]
    wide_ref[:, :rank] = dot_nn(basis, transfer_ref[0]).astype(bf16)
    wide_ref[:, rank:] = basis
    for start in range(0, leaf, step):
        squared = dot_nn(rows_left, right_ref[:, pl.ds(start, step)])
        squared = jnp.maximum(squared, 1e-30)
        root = squared * lax.rsqrt(squared)
        falloff = jnp.exp2(root * rate)
        both_ref[0:rows, pl.ds(start, step)] = ((1.0 + root * slope) * falloff).astype(bf16)
        both_ref[rows : 2 * rows, pl.ds(start, step)] = (squared * falloff).astype(bf16)

    sums = dot_nn(both_ref[...], probes_ref[...])
    kernel_ref[...] = sums[:rows].astype(bf16)
    derivative_ref[...] = (sums[rows:] * (slope * slope)).astype(bf16)


def near_part(order, points, transfer, basis, probes, extra, first, count, rows):
    leaf, columns = probes.shape
    rank = basis.shape[1]
    out_shape = [pltpu.HBM((count * rows, width), bf16) for width in (columns, columns, 2 * rank)]
    out_specs = [pl.BlockSpec((rows, width), lambda i: (i, 0)) for width in (columns, columns, 2 * rank)]
    extra_specs = []
    if extra:
        out_shape.append(pltpu.HBM((2, columns, rank), bf16))
        out_specs.append(pl.BlockSpec((2, columns, rank), lambda i: (0, 0, 0)))
        extra_specs = [smem()] + [
            pl.BlockSpec(array.shape, functools.partial(lambda n, i: (0,) * n, array.ndim)) for array in extra[1:]
        ]
    whole = lambda i: (0, 0)
    return pl.pallas_call(
        functools.partial(near_kernel, first=first),
        grid=(count,),
        out_shape=tuple(out_shape),
        in_specs=[
            pl.BlockSpec(order.shape, whole),
            pl.BlockSpec(points.shape, whole),
            pl.BlockSpec(transfer.shape, lambda i: (0, 0, 0)),
            pl.BlockSpec(basis.shape, whole),
            pl.BlockSpec(memory_space=pltpu.HBM),
        ]
        + extra_specs,
        out_specs=tuple(out_specs),
        scratch_shapes=[
            pltpu.VMEM((128, leaf), bf16),
            pltpu.VMEM((128, leaf), bf16),
            pltpu.VMEM((rows, leaf), bf16),
            pltpu.VMEM((2 * rows, leaf), bf16),
            pltpu.VMEM(probes.shape, bf16),
            pltpu.SemaphoreType.DMA,
        ],
        compiler_params=params(32),
        cost_estimate=cost(2.0 * count * rows * leaf * (columns * 2 + 512), 6 * MIB),
    )(*held_in_hbm(order, points, transfer, basis, probes), *extra)


def fine_up_kernel(lift_ref, transfer_ref, one_ref, two_ref, three_ref):
    twos = []
    for node in range(2):
        total = None
        for child in (2 * node, 2 * node + 1):
            value = lift_ref[2 * child] + lift_ref[2 * child + 1]
            one_ref[child] = value
            moved = exact(dot_nn, value, transfer_ref[0, child])
            total = moved if total is None else total + moved
        two_ref[node] = total
        twos.append(total)
    three_ref[...] = exact(dot_nn, twos[0], transfer_ref[0, 4]) + exact(dot_nn, twos[1], transfer_ref[0, 5])


def fine_up(lifts, transfer):
    columns, rank = lifts.shape[1:]
    return pl.pallas_call(
        fine_up_kernel,
        out_shape=(
            jax.ShapeDtypeStruct((4, columns, rank), f32),
            jax.ShapeDtypeStruct((2, columns, rank), f32),
            jax.ShapeDtypeStruct((columns, rank), f32),
        ),
        in_specs=vmem(2),
        out_specs=tuple(vmem(3)),
        compiler_params=params(8),
        cost_estimate=cost(1e9, MIB),
        name="fine_up",
    )(lifts, transfer)


def pair_up_kernel(place_ref, own_ref, other_ref, transfer_ref, out_ref):
    place = place_ref[0]
    out_ref[...] = exact(dot_nn, own_ref[...], transfer_ref[place]) + exact(
        dot_nn, other_ref[...], transfer_ref[place ^ 1]
    )


def pair_up(place, own, other, transfer):
    return pl.pallas_call(
        pair_up_kernel,
        out_shape=jax.ShapeDtypeStruct(own.shape, f32),
        in_specs=[smem()] + vmem(3),
        out_specs=vmem(1)[0],
        compiler_params=params(8),
        cost_estimate=cost(1e8, MIB // 8),
        name="pair_up",
    )(place, own, other, transfer)


def quad_up_kernel(place_ref, own_ref, x1_ref, x2_ref, x3_ref, transfer_ref, pair_ref, top_ref):
    place = place_ref[0] >> 1
    base = 32
    values = (own_ref, x1_ref, x2_ref, x3_ref)
    moved = [exact(dot_nn, value[...], transfer_ref[base + (place ^ flip)]) for flip, value in enumerate(values)]
    mine = moved[0] + moved[1]
    theirs = moved[2] + moved[3]
    pair_ref[...] = theirs
    place = place >> 1
    base = 48
    top_ref[...] = exact(dot_nn, mine, transfer_ref[base + place]) + exact(
        dot_nn, theirs, transfer_ref[base + (place ^ 1)]
    )


def quad_up(place, own, x1, x2, x3, transfer):
    shape = jax.ShapeDtypeStruct(own.shape, f32)
    return pl.pallas_call(
        quad_up_kernel,
        out_shape=(shape, shape),
        in_specs=[smem()] + vmem(5),
        out_specs=tuple(vmem(2)),
        compiler_params=params(8),
        cost_estimate=cost(1e8, MIB // 8),
        name="quad_up",
    )(place, own, x1, x2, x3, transfer)


def coupled(value, pair_ref, index, side):
    rank = value.shape[1]
    sides = []
    for k in range(2):
        matrix = pair_ref[index, k].astype(f32)
        sides.append(jnp.where(side == 0, jnp.transpose(matrix), matrix).astype(bf16))
    both = exact(dot_nn, value, jnp.concatenate(sides, axis=1))
    return jnp.concatenate([both[:, :rank], both[:, rank:]], axis=0)


def turn_kernel(
    place_ref,
    top_ref,
    x1_ref,
    x2_ref,
    x3_ref,
    five_ref,
    four_ref,
    three_ref,
    two_ref,
    one_ref,
    coarse_ref,
    couple_ref,
    fine_ref,
    fine_couple_ref,
    out_ref,
):
    place = place_ref[0]
    at = place >> 3
    far = exact(dot_nn, x2_ref[...], coarse_ref[56 + (at ^ 2)]) + exact(
        dot_nn, x3_ref[...], coarse_ref[56 + (at ^ 3)]
    )
    z = coupled(far, couple_ref, 30, at >> 1)
    levels = (
        (x1_ref, 28, 56, 3),
        (five_ref, 24, 48, 2),
        (four_ref, 16, 32, 1),
        (three_ref, 0, 0, 0),
    )
    for sibling_ref, couple_base, base, shift in levels:
        at = place >> shift
        g = coupled(sibling_ref[...], couple_ref, couple_base + (at >> 1), at & 1)
        z = g + exact(dot_nt, z, coarse_ref[base + at])
    for node in range(2):
        g = coupled(two_ref[1 - node], fine_couple_ref.at[0], 6, node)
        z_two = g + exact(dot_nt, z, fine_ref[0, 4 + node])
        for child in (2 * node, 2 * node + 1):
            g = coupled(one_ref[child ^ 1], fine_couple_ref.at[0], 4 + node, child & 1)
            z_one = g + exact(dot_nt, z_two, fine_ref[0, child])
            out_ref[2 * child] = z_one
            out_ref[2 * child + 1] = z_one


def turn(place, *operands):
    columns, rank = operands[0].shape
    return pl.pallas_call(
        turn_kernel,
        out_shape=jax.ShapeDtypeStruct((8, 2 * columns, rank), f32),
        in_specs=[smem()] + vmem(len(operands)),
        out_specs=vmem(1)[0],
        compiler_params=params(16),
        cost_estimate=cost(1e9, MIB),
        name="turn",
    )(place, *operands)


def finish_kernel(down_ref, couple_hbm, *refs):
    parts_hbm = refs[:6]
    out_k_hbm, out_d_hbm, couple_ref, wide_ref, near_ref, held_ref, in_sems, out_sems = refs[6:]
    part = down_ref.shape[1] // 2
    arrivals = [pltpu.make_async_copy(couple_hbm, couple_ref, in_sems.at[0])]
    spans = []
    start = 0
    for half in range(2):
        near_k, near_d, wide = parts_hbm[3 * half : 3 * half + 3]
        span = pl.ds(start, near_k.shape[0])
        spans.append(span)
        start += near_k.shape[0]
        for source, target in (
            (wide, wide_ref.at[span, :]),
            (near_k, near_ref.at[0, span, :]),
            (near_d, near_ref.at[1, span, :]),
        ):
            arrivals.append(pltpu.make_async_copy(source, target, in_sems.at[len(arrivals)]))
    for copy in arrivals:
        copy.start()
    parents = [
        jnp.concatenate([down_ref[s, k * part : (k + 1) * part].astype(bf16) for s in range(down_ref.shape[0])], axis=0)
        for k in range(2)
    ]
    arrivals[0].wait()
    both = [jnp.concatenate([parents[k], couple_ref[k]], axis=1) for k in range(2)]
    departures = []
    for half, span in enumerate(spans):
        arrivals[1 + 3 * half].wait()
        for k, out_hbm in enumerate((out_k_hbm, out_d_hbm)):
            arrivals[2 + 3 * half + k].wait()
            far = dot_nt(wide_ref[span, :], both[k])
            held_ref[k, span, :] = (near_ref[k, span, :].astype(f32) + far).astype(bf16)
            departures.append(
                pltpu.make_async_copy(held_ref.at[k, span, :], out_hbm.at[span, :], out_sems.at[len(departures)])
            )
            departures[-1].start()
    for copy in departures:
        copy.wait()


def finish(down, couple, *parts):
    leaf = parts[0].shape[0] + parts[3].shape[0]
    columns = parts[0].shape[1]
    wide = parts[2].shape[1]
    shape = jax.ShapeDtypeStruct((leaf, columns), bf16)
    return pl.pallas_call(
        finish_kernel,
        out_shape=(shape, shape),
        in_specs=vmem(1) + hbm(1 + len(parts)),
        out_specs=tuple(hbm(2)),
        scratch_shapes=[
            pltpu.VMEM(couple.shape, bf16),
            pltpu.VMEM((leaf, wide), bf16),
            pltpu.VMEM((2, leaf, columns), bf16),
            pltpu.VMEM((2, leaf, columns), bf16),
            pltpu.SemaphoreType.DMA((7,)),
            pltpu.SemaphoreType.DMA((4,)),
        ],
        compiler_params=params(24),
        cost_estimate=cost(1e9, 10 * MIB),
        name="finish",
    )(down, *held_in_hbm(couple, *parts))


def swap(x, axis, mask):
    return lax.ppermute(x, axis, [(i, i ^ mask) for i in range(lax.axis_size(axis))])


def per_device(
    points, order, probes, leaf_basis, leaf_transfer, fine_transfer, coarse_transfer, fine_couple, coarse_couple
):
    group = lax.axis_size("gy")
    place = jnp.stack([lax.axis_index("gx"), lax.axis_index("gy")]).astype(jnp.int32)
    points_t = jnp.transpose(points)
    h_t, lift_t = leaf_up(order, leaf_basis, probes, leaf_transfer)
    columns, rank = h_t.shape
    leaf = probes.shape[0]
    order_a, lift_t = lax.optimization_barrier((order, lift_t))
    lifts = lax.all_to_all(lift_t.reshape(group, columns // group, rank), "gy", 0, 0)
    rows = leaf // 16
    near_a = near_part(order_a, points_t, leaf_transfer, leaf_basis, probes, (), 0, 2, 4 * rows)
    near_a, lifts = lax.optimization_barrier((near_a, lifts))
    one, two, three = fine_up(lifts, fine_transfer)
    three_sibling = swap(three, "gx", 1)
    four = pair_up(place, three, three_sibling, coarse_transfer)
    four, h_t = lax.optimization_barrier((four, h_t))
    y1, y2, y3 = [swap(four, "gx", mask << 1) for mask in (1, 2, 3)]
    leaf_sibling = swap(h_t, "gy", 1)
    five_sibling, six = quad_up(place, four, y1, y2, y3, coarse_transfer)
    x1, x2, x3 = [swap(six, "gx", mask << 3) for mask in (1, 2, 3)]
    sent = turn(
        place,
        six,
        x1,
        x2,
        x3,
        five_sibling,
        y1,
        three_sibling,
        two,
        one,
        coarse_transfer,
        coarse_couple,
        fine_transfer,
        fine_couple,
    )
    order_b, leaf_sibling, sent = lax.optimization_barrier((order, leaf_sibling, sent))
    down = lax.all_to_all(sent, "gy", 0, 0)
    extra = (place, leaf_sibling, *held_in_hbm(fine_couple))
    near_b = near_part(order_b, points_t, leaf_transfer, leaf_basis, probes, extra, 8 * rows, 2, 4 * rows)
    return finish(down, near_b[3], *near_a, *near_b[:3])


def solution(mesh):
    placed = (
        P(("gx", "gy"), None),
        P(("gx", "gy"), None),
        P(("gx", "gy"), None),
        P(("gx", "gy"), None),
        P(("gx", "gy"), None, None),
        P("gx", None, None, None),
        P(),
        P("gx", None, None, None, None),
        P(),
    )
    return jax.shard_map(
        per_device,
        mesh=mesh,
        in_specs=placed,
        out_specs=(P(("gx", "gy"), None), P(("gx", "gy"), None)),
        check_vma=False,
    )
```

```python
import functools
import math

import jax
import jax.numpy as jnp
from jax import lax
from jax.experimental import pallas as pl
from jax.experimental.pallas import tpu as pltpu
from jax.sharding import PartitionSpec as P


length_scale = 3.25
bf16 = jnp.bfloat16
f32 = jnp.float32
MIB = 1 << 20


def vmem(count):
    return [pl.BlockSpec(memory_space=pltpu.VMEM)] * count


def held_in_hbm(*arrays):
    return [pltpu.with_memory_space_constraint(array, pltpu.HBM) for array in arrays]


def hbm(count):
    return [pl.BlockSpec(memory_space=pltpu.HBM)] * count


def smem():
    return pl.BlockSpec(memory_space=pltpu.SMEM)


def params(mib):
    return pltpu.CompilerParams(vmem_limit_bytes=mib * MIB)


def cost(flops, moved):
    return pl.CostEstimate(flops=int(flops), bytes_accessed=int(moved), transcendentals=0)


def dot_nn(a, b):
    return lax.dot_general(a, b, (((1,), (0,)), ((), ())), preferred_element_type=f32)


def dot_nt(a, b):
    return lax.dot_general(a, b, (((1,), (1,)), ((), ())), preferred_element_type=f32)


def split(x):
    high = x.astype(bf16)
    low = (x - high.astype(f32)).astype(bf16)
    return jnp.concatenate([high, low], axis=0)


def exact(dot, x, w):
    rows = x.shape[0]
    both = dot(split(x), w)
    return both[:rows] + both[rows:]


def order_columns(order_ref, start, rows):
    pieces = []
    for piece in range(rows // 128):
        line = order_ref[0:1, pl.ds(start + piece * 128, 128)]
        pieces.append(jnp.transpose(jnp.broadcast_to(line, (128, 128))))
    return jnp.concatenate(pieces, axis=0).astype(jnp.int16)


def one_hot(columns, start, width):
    lane = lax.broadcasted_iota(jnp.int32, columns.shape, 1)
    tiles = []
    for tile in range(width // 128):
        lanes = (lane + (start + tile * 128)).astype(jnp.int16)
        tiles.append(jnp.where(columns == lanes, bf16(1.0), bf16(0.0)))
    return jnp.concatenate(tiles, axis=1)


def leaf_up_kernel(
    order_hbm,
    basis_hbm,
    probes_hbm,
    transfer_hbm,
    h_ref,
    lift_ref,
    order_ref,
    basis_ref,
    probes_ref,
    transfer_ref,
    columns_ref,
    hot_ref,
    stored_ref,
    sems,
):
    copies = [
        pltpu.make_async_copy(source, target, sems.at[n])
        for n, (source, target) in enumerate(
            (
                (order_hbm, order_ref),
                (basis_hbm, basis_ref),
                (probes_hbm, probes_ref),
                (transfer_hbm, transfer_ref),
            )
        )
    ]
    for copy in copies:
        copy.start()
    leaf = basis_ref.shape[0]
    step = 512
    copies[0].wait()
    columns_ref[...] = order_columns(order_ref, 0, leaf)
    copies[1].wait()
    basis_t = jnp.transpose(basis_ref[...])
    for start in range(0, leaf, step):
        hot_ref[:, pl.ds(start, step)] = one_hot(columns_ref[...], start, step)
        stored_ref[:, pl.ds(start, step)] = dot_nn(basis_t, hot_ref[:, pl.ds(start, step)]).astype(bf16)
    copies[2].wait()
    h_t = jnp.transpose(dot_nn(stored_ref[...], probes_ref[...]))
    copies[3].wait()
    h_ref[...] = h_t
    half = h_t.shape[0] // 2
    for part in (0, half):
        lift_ref[part : part + half, :] = exact(dot_nn, h_t[part : part + half], transfer_ref[0])


def leaf_up(order, basis, probes, transfer):
    leaf, rank = basis.shape
    columns = probes.shape[1]
    shape = jax.ShapeDtypeStruct((columns, rank), f32)
    return pl.pallas_call(
        leaf_up_kernel,
        out_shape=(shape, shape),
        in_specs=hbm(4),
        out_specs=tuple(vmem(2)),
        scratch_shapes=[
            pltpu.VMEM(order.shape, order.dtype),
            pltpu.VMEM(basis.shape, bf16),
            pltpu.VMEM(probes.shape, bf16),
            pltpu.VMEM(transfer.shape, bf16),
            pltpu.VMEM((leaf, 128), jnp.int16),
            pltpu.VMEM((leaf, leaf), bf16),
            pltpu.VMEM((rank, leaf), bf16),
            pltpu.SemaphoreType.DMA((4,)),
        ],
        compiler_params=params(24),
        cost_estimate=cost(4e9, 3 * MIB),
        name="leaf_up",
    )(*held_in_hbm(order, basis, probes, transfer))


def near_kernel(order_ref, points_ref, transfer_ref, basis_ref, probes_hbm, *refs, first):
    extra = refs[:3] if len(refs) > 10 else None
    outs, (right_ref, left_ref, hot_ref, both_ref, probes_ref, sem) = refs[:-6], refs[-6:]
    kernel_ref, derivative_ref, wide_ref = outs[len(outs) - 3 :] if extra is None else outs[3:6]
    features, leaf = points_ref.shape
    rows = kernel_ref.shape[0]
    step = 256
    slope = math.sqrt(3.0) / length_scale
    rate = -slope * math.log2(math.e)
    block = pl.program_id(0)
    copy = pltpu.make_async_copy(probes_hbm, probes_ref, sem)

    @pl.when(block == 0)
    def _():
        copy.start()
        values = points_ref[...].astype(f32)
        norm = jnp.sum(values * values, axis=0, keepdims=True)
        high = norm.astype(bf16).astype(f32)
        rest = norm - high
        middle = rest.astype(bf16).astype(f32)
        low = rest - middle
        line = lax.broadcasted_iota(jnp.int32, (128 - features, leaf), 0)

        def tail(norm_line, ones_line):
            ones = (line >= ones_line) & (line < ones_line + 3)
            out = jnp.where(ones, 1.0, 0.0)
            for offset, piece in enumerate((high, middle, low)):
                out = jnp.where(line == norm_line + offset, piece, out)
            return out

        right_ref[...] = jnp.concatenate([values, tail(0, 3)], axis=0).astype(bf16)
        left_ref[...] = jnp.concatenate([-2.0 * values, tail(3, 0)], axis=0).astype(bf16)
        if extra is not None:
            place_ref, sibling_ref, couple_ref = extra
            place = place_ref[1]
            size = sibling_ref.shape[0]
            g = coupled(sibling_ref[...], couple_ref.at[0], place >> 1, place & 1).astype(bf16)
            outs[6][0] = g[:size]
            outs[6][1] = g[size:]

    columns = order_columns(order_ref, first + block * rows, rows)
    hot_ref[...] = one_hot(columns, 0, leaf)
    half = rows // 2
    rows_left = jnp.concatenate(
        [dot_nt(hot_ref[part : part + half, :], left_ref[...]) for part in (0, half)], axis=0
    ).astype(bf16)

    @pl.when(block == 0)
    def _():
        copy.wait()

    basis = basis_ref[pl.ds(pl.multiple_of(first + block * rows, 128), rows), :]
    rank = basis.shape[1]
    wide_ref[:, :rank] = dot_nn(basis, transfer_ref[0]).astype(bf16)
    wide_ref[:, rank:] = basis
    for start in range(0, leaf, step):
        squared = dot_nn(rows_left, right_ref[:, pl.ds(start, step)])
        squared = jnp.maximum(squared, 1e-30)
        root = squared * lax.rsqrt(squared)
        falloff = jnp.exp2(root * rate)
        both_ref[0:rows, pl.ds(start, step)] = ((1.0 + root * slope) * falloff).astype(bf16)
        both_ref[rows : 2 * rows, pl.ds(start, step)] = (squared * falloff).astype(bf16)

    sums = dot_nn(both_ref[...], probes_ref[...])
    kernel_ref[...] = sums[:rows].astype(bf16)
    derivative_ref[...] = (sums[rows:] * (slope * slope)).astype(bf16)


def near_part(order, points, transfer, basis, probes, extra, first, count, rows):
    leaf, columns = probes.shape
    rank = basis.shape[1]
    out_shape = [pltpu.HBM((count * rows, width), bf16) for width in (columns, columns, 2 * rank)]
    out_specs = [pl.BlockSpec((rows, width), lambda i: (i, 0)) for width in (columns, columns, 2 * rank)]
    extra_specs = []
    if extra:
        out_shape.append(pltpu.HBM((2, columns, rank), bf16))
        out_specs.append(pl.BlockSpec((2, columns, rank), lambda i: (0, 0, 0)))
        extra_specs = [smem()] + [
            pl.BlockSpec(array.shape, functools.partial(lambda n, i: (0,) * n, array.ndim)) for array in extra[1:]
        ]
    whole = lambda i: (0, 0)
    return pl.pallas_call(
        functools.partial(near_kernel, first=first),
        grid=(count,),
        out_shape=tuple(out_shape),
        in_specs=[
            pl.BlockSpec(order.shape, whole),
            pl.BlockSpec(points.shape, whole),
            pl.BlockSpec(transfer.shape, lambda i: (0, 0, 0)),
            pl.BlockSpec(basis.shape, whole),
            pl.BlockSpec(memory_space=pltpu.HBM),
        ]
        + extra_specs,
        out_specs=tuple(out_specs),
        scratch_shapes=[
            pltpu.VMEM((128, leaf), bf16),
            pltpu.VMEM((128, leaf), bf16),
            pltpu.VMEM((rows, leaf), bf16),
            pltpu.VMEM((2 * rows, leaf), bf16),
            pltpu.VMEM(probes.shape, bf16),
            pltpu.SemaphoreType.DMA,
        ],
        compiler_params=params(32),
        cost_estimate=cost(2.0 * count * rows * leaf * (columns * 2 + 512), 6 * MIB),
    )(order, points, transfer, *held_in_hbm(basis, probes), *extra)


def fine_up_kernel(lift_ref, transfer_ref, one_ref, two_ref, three_ref):
    twos = []
    for node in range(2):
        total = None
        for child in (2 * node, 2 * node + 1):
            value = lift_ref[2 * child] + lift_ref[2 * child + 1]
            one_ref[child] = value
            moved = exact(dot_nn, value, transfer_ref[0, child])
            total = moved if total is None else total + moved
        two_ref[node] = total
        twos.append(total)
    three_ref[...] = exact(dot_nn, twos[0], transfer_ref[0, 4]) + exact(dot_nn, twos[1], transfer_ref[0, 5])


def fine_up(lifts, transfer):
    columns, rank = lifts.shape[1:]
    return pl.pallas_call(
        fine_up_kernel,
        out_shape=(
            jax.ShapeDtypeStruct((4, columns, rank), f32),
            jax.ShapeDtypeStruct((2, columns, rank), f32),
            jax.ShapeDtypeStruct((columns, rank), f32),
        ),
        in_specs=vmem(2),
        out_specs=tuple(vmem(3)),
        compiler_params=params(8),
        cost_estimate=cost(1e9, MIB),
        name="fine_up",
    )(lifts, transfer)


def pair_up_kernel(place_ref, own_ref, other_ref, transfer_ref, out_ref):
    place = place_ref[0]
    out_ref[...] = exact(dot_nn, own_ref[...], transfer_ref[place]) + exact(
        dot_nn, other_ref[...], transfer_ref[place ^ 1]
    )


def pair_up(place, own, other, transfer):
    return pl.pallas_call(
        pair_up_kernel,
        out_shape=jax.ShapeDtypeStruct(own.shape, f32),
        in_specs=[smem()] + vmem(3),
        out_specs=vmem(1)[0],
        compiler_params=params(8),
        cost_estimate=cost(1e8, MIB // 8),
        name="pair_up",
    )(place, own, other, transfer)


def quad_up_kernel(place_ref, own_ref, x1_ref, x2_ref, x3_ref, transfer_ref, pair_ref, top_ref):
    place = place_ref[0] >> 1
    base = 32
    values = (own_ref, x1_ref, x2_ref, x3_ref)
    moved = [exact(dot_nn, value[...], transfer_ref[base + (place ^ flip)]) for flip, value in enumerate(values)]
    mine = moved[0] + moved[1]
    theirs = moved[2] + moved[3]
    pair_ref[...] = theirs
    place = place >> 1
    base = 48
    top_ref[...] = exact(dot_nn, mine, transfer_ref[base + place]) + exact(
        dot_nn, theirs, transfer_ref[base + (place ^ 1)]
    )


def quad_up(place, own, x1, x2, x3, transfer):
    shape = jax.ShapeDtypeStruct(own.shape, f32)
    return pl.pallas_call(
        quad_up_kernel,
        out_shape=(shape, shape),
        in_specs=[smem()] + vmem(5),
        out_specs=tuple(vmem(2)),
        compiler_params=params(8),
        cost_estimate=cost(1e8, MIB // 8),
        name="quad_up",
    )(place, own, x1, x2, x3, transfer)


def coupled(value, pair_ref, index, side):
    rank = value.shape[1]
    sides = []
    for k in range(2):
        matrix = pair_ref[index, k].astype(f32)
        sides.append(jnp.where(side == 0, jnp.transpose(matrix), matrix).astype(bf16))
    both = exact(dot_nn, value, jnp.concatenate(sides, axis=1))
    return jnp.concatenate([both[:, :rank], both[:, rank:]], axis=0)


def turn_kernel(
    place_ref,
    top_ref,
    x1_ref,
    x2_ref,
    x3_ref,
    five_ref,
    four_ref,
    three_ref,
    two_ref,
    one_ref,
    coarse_ref,
    couple_ref,
    fine_ref,
    fine_couple_ref,
    out_ref,
):
    place = place_ref[0]
    at = place >> 3
    far = exact(dot_nn, x2_ref[...], coarse_ref[56 + (at ^ 2)]) + exact(
        dot_nn, x3_ref[...], coarse_ref[56 + (at ^ 3)]
    )
    z = coupled(far, couple_ref, 30, at >> 1)
    levels = (
        (x1_ref, 28, 56, 3),
        (five_ref, 24, 48, 2),
        (four_ref, 16, 32, 1),
        (three_ref, 0, 0, 0),
    )
    for sibling_ref, couple_base, base, shift in levels:
        at = place >> shift
        g = coupled(sibling_ref[...], couple_ref, couple_base + (at >> 1), at & 1)
        z = g + exact(dot_nt, z, coarse_ref[base + at])
    for node in range(2):
        g = coupled(two_ref[1 - node], fine_couple_ref.at[0], 6, node)
        z_two = g + exact(dot_nt, z, fine_ref[0, 4 + node])
        for child in (2 * node, 2 * node + 1):
            g = coupled(one_ref[child ^ 1], fine_couple_ref.at[0], 4 + node, child & 1)
            z_one = g + exact(dot_nt, z_two, fine_ref[0, child])
            out_ref[2 * child] = z_one
            out_ref[2 * child + 1] = z_one


def turn(place, *operands):
    columns, rank = operands[0].shape
    return pl.pallas_call(
        turn_kernel,
        out_shape=jax.ShapeDtypeStruct((8, 2 * columns, rank), f32),
        in_specs=[smem()] + vmem(len(operands)),
        out_specs=vmem(1)[0],
        compiler_params=params(16),
        cost_estimate=cost(1e9, MIB),
        name="turn",
    )(place, *operands)


def finish_kernel(down_ref, couple_hbm, *refs):
    parts_hbm = refs[:6]
    out_k_hbm, out_d_hbm, couple_ref, wide_ref, near_ref, held_ref, in_sems, out_sems = refs[6:]
    part = down_ref.shape[1] // 2
    arrivals = [pltpu.make_async_copy(couple_hbm, couple_ref, in_sems.at[0])]
    spans = []
    for half in (1, 0):
        near_k, near_d, wide = parts_hbm[3 * half : 3 * half + 3]
        span = pl.ds(half * parts_hbm[0].shape[0], near_k.shape[0])
        spans.append(span)
        for source, target in (
            (wide, wide_ref.at[span, :]),
            (near_k, near_ref.at[0, span, :]),
            (near_d, near_ref.at[1, span, :]),
        ):
            arrivals.append(pltpu.make_async_copy(source, target, in_sems.at[len(arrivals)]))
    for copy in arrivals:
        copy.start()
    parents = [
        jnp.concatenate([down_ref[s, k * part : (k + 1) * part].astype(bf16) for s in range(down_ref.shape[0])], axis=0)
        for k in range(2)
    ]
    arrivals[0].wait()
    both = [jnp.concatenate([parents[k], couple_ref[k]], axis=1) for k in range(2)]
    departures = []
    for half, span in enumerate(spans):
        arrivals[1 + 3 * half].wait()
        for k, out_hbm in enumerate((out_k_hbm, out_d_hbm)):
            arrivals[2 + 3 * half + k].wait()
            far = dot_nt(wide_ref[span, :], both[k])
            held_ref[k, span, :] = (near_ref[k, span, :].astype(f32) + far).astype(bf16)
            departures.append(
                pltpu.make_async_copy(held_ref.at[k, span, :], out_hbm.at[span, :], out_sems.at[len(departures)])
            )
            departures[-1].start()
    for copy in departures:
        copy.wait()


def finish(down, couple, *parts):
    leaf = parts[0].shape[0] + parts[3].shape[0]
    columns = parts[0].shape[1]
    wide = parts[2].shape[1]
    shape = jax.ShapeDtypeStruct((leaf, columns), bf16)
    return pl.pallas_call(
        finish_kernel,
        out_shape=(shape, shape),
        in_specs=vmem(1) + hbm(1 + len(parts)),
        out_specs=tuple(hbm(2)),
        scratch_shapes=[
            pltpu.VMEM(couple.shape, bf16),
            pltpu.VMEM((leaf, wide), bf16),
            pltpu.VMEM((2, leaf, columns), bf16),
            pltpu.VMEM((2, leaf, columns), bf16),
            pltpu.SemaphoreType.DMA((7,)),
            pltpu.SemaphoreType.DMA((4,)),
        ],
        compiler_params=params(24),
        cost_estimate=cost(1e9, 10 * MIB),
        name="finish",
    )(down, *held_in_hbm(couple, *parts))


def swap(x, axis, mask):
    return lax.ppermute(x, axis, [(i, i ^ mask) for i in range(lax.axis_size(axis))])


def per_device(
    points, order, probes, leaf_basis, leaf_transfer, fine_transfer, coarse_transfer, fine_couple, coarse_couple
):
    group = lax.axis_size("gy")
    place = jnp.stack([lax.axis_index("gx"), lax.axis_index("gy")]).astype(jnp.int32)
    points_t = jnp.transpose(points)
    h_t, lift_t = leaf_up(order, leaf_basis, probes, leaf_transfer)
    columns, rank = h_t.shape
    leaf = probes.shape[0]
    order_a, lift_t = lax.optimization_barrier((order, lift_t))
    lifts = lax.all_to_all(lift_t.reshape(group, columns // group, rank), "gy", 0, 0)
    rows = leaf // 16
    near_a = near_part(order_a, points_t, leaf_transfer, leaf_basis, probes, (), 0, 2, 3 * rows)
    near_a, lifts = lax.optimization_barrier((near_a, lifts))
    one, two, three = fine_up(lifts, fine_transfer)
    three_sibling = swap(three, "gx", 1)
    four = pair_up(place, three, three_sibling, coarse_transfer)
    four, h_t = lax.optimization_barrier((four, h_t))
    y1, y2, y3 = [swap(four, "gx", mask << 1) for mask in (1, 2, 3)]
    leaf_sibling = swap(h_t, "gy", 1)
    five_sibling, six = quad_up(place, four, y1, y2, y3, coarse_transfer)
    x1, x2, x3 = [swap(six, "gx", mask << 3) for mask in (1, 2, 3)]
    sent = turn(
        place,
        six,
        x1,
        x2,
        x3,
        five_sibling,
        y1,
        three_sibling,
        two,
        one,
        coarse_transfer,
        coarse_couple,
        fine_transfer,
        fine_couple,
    )
    order_b, leaf_sibling, sent = lax.optimization_barrier((order, leaf_sibling, sent))
    down = lax.all_to_all(sent, "gy", 0, 0)
    extra = (place, leaf_sibling, *held_in_hbm(fine_couple))
    near_b = near_part(order_b, points_t, leaf_transfer, leaf_basis, probes, extra, 6 * rows, 2, 5 * rows)
    return finish(down, near_b[3], *near_a, *near_b[:3])


def solution(mesh):
    placed = (
        P(("gx", "gy"), None),
        P(("gx", "gy"), None),
        P(("gx", "gy"), None),
        P(("gx", "gy"), None),
        P(("gx", "gy"), None, None),
        P("gx", None, None, None),
        P(),
        P("gx", None, None, None, None),
        P(),
    )
    return jax.shard_map(
        per_device,
        mesh=mesh,
        in_specs=placed,
        out_specs=(P(("gx", "gy"), None), P(("gx", "gy"), None)),
        check_vma=False,
    )
```
